128 devices in a mesh: row: 8 (over y, x_lo), col: 16 (over x_hi, z, core).
Axes of the slice: x: 4 (x_hi: 2, x_lo: 2; x = x_hi * 2 + x_lo), y: 4, z: 4, core: 2. Of those that a mesh axis runs over, the one named last changes fastest.
Arguments:
- u_field: float32 [256, 16384], P('row', 'col'), may hold values from -4 to 4
- v_field: float32 [256, 16384], P('row', 'col'), may hold values from -7.5 to 7.5
- stimulus: float32 [256, 16384], P('row', 'col'), may hold values from -6 to 6
Outputs:
- u_final: float32 [256, 16384], P('row', 'col')
- v_final: float32 [256, 16384], P('row', 'col')
The draws below stay inside these ranges and needn't reach their ends.
All inputs are finite; a program needn't handle non-finite values.
Results may differ from the reference program's by a relative error of at most 0.0003.
Values sent between devices are 32-bit elements; how exact they have to be, the bound alone decides.
A program may use at most 64 MiB of HBM per device.

```python
import jax
import jax.numpy as jnp
from jax import lax

MICRO_COUNT = 4
MIDDLE = 3
TOP = 3
OUTER = 2
NROWS = 256
NCOLS = 16384


def draw_v_field(key, part):
    first_key, second_key, third_key = jax.random.split(key, 3)
    row_stripes = (NROWS + 7) // 8
    col_stripes = (NCOLS + 7) // 8
    row_levels = jax.random.uniform(first_key, (row_stripes,), minval=-3.0, maxval=3.0)
    col_levels = jax.random.uniform(second_key, (col_stripes,), minval=-3.0, maxval=3.0)
    roughness = 0.5 * jax.random.truncated_normal(third_key, -3.0, 3.0, (NROWS, NCOLS))
    row_index = jnp.arange(NROWS) // 8
    col_index = jnp.arange(NCOLS) // 8
    combined = row_levels[row_index][:, None] + col_levels[col_index][None, :] + roughness
    return combined.astype(jnp.float32)


def levels(rng, shape, cuts, least, largest):
    loudness = 1.0
    for position, shards_of in cuts:
        draws = jax.random.uniform(jax.random.fold_in(jax.random.fold_in(rng, 6), position), (shards_of,), jnp.float32, least / len(cuts), largest / len(cuts))
        loudness = loudness * jnp.repeat(jnp.exp(draws), shape[position] // shards_of).reshape((-1,) + (1,) * (len(shape) - 1 - position))
    return loudness


def centred(own_key, dims, scale, reach, shards=(), kind=jnp.bfloat16):
    entries = scale * jax.random.normal(own_key, dims, jnp.float32)
    if shards:
        entries = entries * levels(own_key, dims, shards, -0.22, 0.18)
    return jnp.clip(entries, -reach, reach).astype(kind)


def setup_inputs(seed: int = 0) -> dict:
    seeds = jax.random.split(jax.random.key(seed), 4)
    return {
        "u_field": centred(seeds[0], (NROWS, NCOLS), 1.0, 4.0, ((0, 8), (1, 16)), jnp.float32),
        "v_field": draw_v_field(jax.random.fold_in(seeds[3], 71), 0),
        "stimulus": centred(seeds[2], (NROWS, NCOLS), 0.5, 6.0, ((0, 8), (1, 16)), jnp.float32),
    }


RATE_U = 0.125
RATE_V = 0.125
TIME_STEP = 0.05
RECOVERY = 0.08
OFFSET = 0.7
DAMPING = 0.8


def neighbours(grid):
    total = jnp.roll(grid, 1, 0) + jnp.roll(grid, -1, 0)
    total = total + jnp.roll(grid, 1, 1) + jnp.roll(grid, -1, 1)
    return total - 4.0 * grid


def advance(fields, stimulus):
    u_now, v_now = fields
    u_next = u_now + RATE_U * neighbours(u_now) + TIME_STEP * (u_now - u_now * u_now * u_now / 3.0 - v_now + stimulus)
    v_next = v_now + RATE_V * neighbours(v_now) + TIME_STEP * RECOVERY * (u_now + OFFSET - DAMPING * v_now)
    return (u_next, v_next)


def forward_linear_jump(inner, repeats):
    def run(fields):
        def turn(present_index, pair_now):
            return (pair_now[1], inner(pair_now[1]))
        previous_fields, latest = lax.fori_loop(0, repeats, turn, (fields, fields))
        return jax.tree.map(lambda last, prior: last + (last - prior), latest, previous_fields)
    return run


def reference(u_field, v_field, stimulus):
    def euler_micro_update(fields):
        return advance(fields, stimulus)
    coarse_state_vector = forward_linear_jump(euler_micro_update, MICRO_COUNT)
    second = forward_linear_jump(coarse_state_vector, MIDDLE)
    third = forward_linear_jump(second, TOP)
    final_fields = lax.fori_loop(0, OUTER, lambda present_index, fields: third(fields), (u_field, v_field))
    return final_fields[0], final_fields[1]
```

```python
import jax
import jax.numpy as jnp
from jax import lax
from jax.experimental import pallas as pl
from jax.experimental.pallas import tpu as pltpu
from jax.sharding import PartitionSpec as P

MESH = pl.DeviceIdType.MESH

MICRO_COUNT = 4
MIDDLE = 3
TOP = 3
OUTER = 2

SCALE = 7.5**0.5
SHIFT = 0.875
KEEP_U = 4.4
KEEP_V = 3.9744
COUPLE = 0.0128

STRIP = 128
HALO = 40
STEPS = TOP * MIDDLE * MICRO_COUNT
WIDE = STRIP + 2 * HALO


def place(chip, core):
    group, spot = lax.div(chip, 8), lax.rem(chip, 8)
    half = lax.div(spot, 4)
    y = half * (7 - spot) + (1 - half) * spot
    x = lax.rem(half + lax.div(group, 4) + lax.rem(group, 4), 2)
    return (2 * y + x, 2 * group + core)


def fine(src, stim, dst, low, count, kind, previous=None, before=None):
    u0 = src[0, low : low + count, :]
    u1 = src[1, low : low + count, :]
    v0 = src[2, low : low + count, :]
    v1 = src[3, low : low + count, :]

    def column(i):
        return src[i, low - 1 : low - 1 + count, :] + src[i, low + 1 : low + 1 + count, :]

    keep_u, keep_v, rate = KEEP_U, KEEP_V, 0.125
    if kind > 0:
        keep_u, keep_v, rate = KEEP_U - 4.0, KEEP_V - 4.0, 0.125 * 2**kind
    su0 = column(0) + (u1 + pltpu.roll(u1, 1, 1))
    su1 = column(1) + (u0 + pltpu.roll(u0, 127, 1))
    sv0 = column(2) + (v1 + pltpu.roll(v1, 1, 1))
    sv1 = column(3) + (v0 + pltpu.roll(v0, 127, 1))
    s0 = stim[4, low : low + count, :]
    s1 = stim[5, low : low + count, :]
    new = [
        (su0 + u0 * (keep_u - u0 * u0)) + (s0 - v0),
        (su1 + u1 * (keep_u - u1 * u1)) + (s1 - v1),
        sv0 + (keep_v * v0 + COUPLE * u0),
        sv1 + (keep_v * v1 + COUPLE * u1),
    ]
    for i in range(4):
        value = new[i] if rate == 1.0 else rate * new[i]
        if kind == 2:
            value = value - previous[i, low : low + count, :]
        if kind == 3:
            twice = previous[i, low : low + count, :]
            value = value - (twice + twice) - before[i, low : low + count, :]
        dst[i, low : low + count, :] = value


def kernel(
    u_in, v_in, s_in, u_out, v_out,
    loaded, rows, first, second, ping, pong, t_one, t_two, y_one, y_two, last, result,
    load_sem, in_send, in_recv, halo_send, halo_recv, out_send, out_recv,
):
    row, col = lax.axis_index("row"), lax.axis_index("col")
    y, x = lax.div(row, 2), lax.rem(row, 2)
    group, core = lax.div(col, 2), lax.rem(col, 2)
    turned = lax.rem(lax.div(group, 4) + lax.rem(group, 4), 2)
    half = lax.rem(x + turned, 2)
    spot = half * (7 - y) + (1 - half) * y
    chip = 8 * group + spot
    own = half * (6 - 2 * y) + (1 - half) * 2 * y + core
    here = half == core
    across = lax.rem(core + turned, 2)

    inputs = (u_in, v_in, s_in)
    loads = [
        pltpu.make_async_copy(inputs[i], loaded.at[i], load_sem.at[i]) for i in range(3)
    ]
    for load in loads:
        load.start()

    left = place(lax.rem(chip + 63 + core, 64), 1 - core)
    right = place(lax.rem(chip + core, 64), 1 - core)

    def target(i):
        to_y = lax.rem(y + (2, 1, 3, 0)[i // 2], 4)
        to_core = lax.rem(core + 1 + i, 2)
        tile = core * (6 - 2 * to_y) + (1 - core) * 2 * to_y + to_core
        return (2 * to_y + across, 2 * group + to_core), tile

    def source(i):
        return lax.rem(row + i, 8)

    barrier = pltpu.get_barrier_semaphore()

    def greet(device):
        pl.semaphore_signal(barrier, inc=1, device_id=device, device_id_type=MESH)

    for i in range(7):
        greet(target(i)[0])
        greet((source(i + 1), 2 * group + half))

    @pl.when(jnp.logical_not(here))
    def _():
        greet(target(7)[0])
        greet((source(0), 2 * group + half))

    greet(left)
    greet(right)
    pl.semaphore_wait(barrier, 16 + 2 * (1 - jnp.where(here, 1, 0)))

    def lanes(tile):
        return pl.ds(pl.multiple_of(tile * 128, 128), 128)

    def piece(where):
        return pl.ds(pl.multiple_of(where * 32, 32), 32)

    def moved_in(field, i):
        device, tile = target(i)
        return pltpu.make_async_remote_copy(
            src_ref=loaded.at[field, :, lanes(tile)],
            dst_ref=rows.at[field, piece(row)],
            send_sem=in_send.at[field, i],
            recv_sem=in_recv.at[field, row],
            device_id=device,
            device_id_type=MESH,
        )

    def kept_in(field):
        return pltpu.make_async_copy(
            inputs[field].at[:, lanes(own)], rows.at[field, piece(row)], in_recv.at[field, row]
        )

    for field in range(3):
        loads[field].wait()
        for i in range(7):
            moved_in(field, i).start()

        @pl.when(here)
        def _():
            kept_in(field).start()

        @pl.when(jnp.logical_not(here))
        def _():
            moved_in(field, 7).start()

    def edge(buffer, planes, which, side):
        mine, theirs = ((HALO, WIDE - HALO), (WIDE - 2 * HALO, 0))[side]
        return pltpu.make_async_remote_copy(
            src_ref=buffer.at[planes, pl.ds(mine, HALO)],
            dst_ref=buffer.at[planes, pl.ds(theirs, HALO)],
            send_sem=halo_send.at[which, side],
            recv_sem=halo_recv.at[which, side],
            device_id=(left, right)[side],
            device_id_type=MESH,
        )

    edges = []
    for field in range(3):
        for sender in range(8):
            pltpu.make_async_copy(
                inputs[field].at[:, pl.ds(0, 128)],
                rows.at[field, pl.ds(32 * sender, 32)],
                in_recv.at[field, sender],
            ).wait()
        for parity in range(2):
            block = rows[field, pl.ds(parity, 128, stride=2), :].T
            if field == 0:
                block = block * (1.0 / SCALE)
            else:
                block = (block - SHIFT) * (0.4 / SCALE)
            first[2 * field + parity, HALO : HALO + STRIP, :] = block
        for side in range(2):
            copy = edge(first, pl.ds(2 * field, 2), field, side)
            copy.start()
            edges.append(copy)
    for copy in edges:
        copy.wait()

    start = first
    for outer in range(OUTER):
        done = 0
        state = start
        goal = (second, last)[outer]
        for top in range(TOP):
            for middle in range(MIDDLE):
                end = (t_one, t_two, (y_one, y_two, goal)[top])[middle]
                for micro in range(MICRO_COUNT):
                    done += 1
                    low = HALO - STEPS + done
                    count = -(-(WIDE - 2 * low) // 8) * 8
                    ends = micro == MICRO_COUNT - 1
                    kind = 0
                    if ends:
                        kind = 1 + (middle == MIDDLE - 1) * (1 + (top == TOP - 1))
                    into = end if ends else (ping, pong)[micro % 2]
                    fine(state, first, into, low, count, kind, t_two, y_two)
                    state = into
        start = goal
        if outer < OUTER - 1:
            edges = [edge(second, pl.ds(0, 4), 3 + outer, side) for side in range(2)]
            for copy in edges:
                copy.start()
            for copy in edges:
                copy.wait()

    outputs = (u_out, v_out)

    def moved_out(field, i):
        to = source(i)
        return pltpu.make_async_remote_copy(
            src_ref=result.at[field, piece(to)],
            dst_ref=outputs[field].at[:, lanes(own)],
            send_sem=out_send.at[field, i],
            recv_sem=out_recv.at[field, own],
            device_id=(to, 2 * group + half),
            device_id_type=MESH,
        )

    for field in range(2):
        for parity in range(2):
            block = last[2 * field + parity, HALO : HALO + STRIP, :]
            if field == 0:
                block = block * SCALE
            else:
                block = block * (SCALE / 0.4) + SHIFT
            result[field, pl.ds(parity, 128, stride=2), :] = block.T
        for i in range(1, 8):
            moved_out(field, i).start()

        @pl.when(jnp.logical_not(here))
        def _():
            moved_out(field, 0).start()

        @pl.when(here)
        def _():
            outputs[field][:, lanes(own)] = result[field, piece(row), :]

    def arrived(field, tile):
        return pltpu.make_async_copy(
            result.at[field, pl.ds(0, 32)],
            outputs[field].at[:, pl.ds(0, 128)],
            out_recv.at[field, tile],
        )

    for field in range(2):
        for tile in range(8):

            @pl.when(jnp.logical_not(here) | (own != tile))
            def _():
                arrived(field, tile).wait()

    for field in range(3):
        for i in range(7):
            moved_in(field, i).wait_send()

        @pl.when(jnp.logical_not(here))
        def _():
            moved_in(field, 7).wait_send()

    for field in range(2):
        for i in range(1, 8):
            moved_out(field, i).wait_send()

        @pl.when(jnp.logical_not(here))
        def _():
            moved_out(field, 0).wait_send()


def body(u_field, v_field, stimulus):
    block = u_field.shape
    state = pltpu.VMEM((4, WIDE, 128), jnp.float32)
    return pl.pallas_call(
        kernel,
        out_shape=[jax.ShapeDtypeStruct(block, jnp.float32)] * 2,
        in_specs=[pl.BlockSpec(memory_space=pl.ANY)] * 3,
        out_specs=[pl.BlockSpec(memory_space=pltpu.VMEM)] * 2,
        scratch_shapes=[
            pltpu.VMEM((3,) + block, jnp.float32),
            pltpu.VMEM((3, 256, STRIP), jnp.float32),
            pltpu.VMEM((6, WIDE, 128), jnp.float32),
            *[state] * 8,
            pltpu.VMEM((2, 256, STRIP), jnp.float32),
            pltpu.SemaphoreType.DMA((3,)),
            pltpu.SemaphoreType.DMA((3, 8)),
            pltpu.SemaphoreType.DMA((3, 8)),
            pltpu.SemaphoreType.DMA((4, 2)),
            pltpu.SemaphoreType.DMA((4, 2)),
            pltpu.SemaphoreType.DMA((2, 8)),
            pltpu.SemaphoreType.DMA((2, 8)),
        ],
        compiler_params=pltpu.CompilerParams(collective_id=0, has_side_effects=True),
    )(u_field, v_field, stimulus)


def solution(mesh):
    return jax.shard_map(
        body,
        mesh=mesh,
        in_specs=(P("row", "col"), P("row", "col"), P("row", "col")),
        out_specs=(P("row", "col"), P("row", "col")),
        check_vma=False,
    )
```

```python
import jax
import jax.numpy as jnp
from jax import lax
from jax.experimental import pallas as pl
from jax.experimental.pallas import tpu as pltpu
from jax.sharding import PartitionSpec as P

MESH = pl.DeviceIdType.MESH

MICRO_COUNT = 4
MIDDLE = 3
TOP = 3
OUTER = 2

SCALE = 7.5**0.5
SHIFT = 0.875
KEEP_U = 4.4
KEEP_V = 3.9744
COUPLE = 0.0128

STRIP = 128
HALO = 40
STEPS = TOP * MIDDLE * MICRO_COUNT
WIDE = STRIP + 2 * HALO


def place(chip, core):
    group, spot = lax.div(chip, 8), lax.rem(chip, 8)
    half = lax.div(spot, 4)
    y = half * (spot - 4) + (1 - half) * (3 - spot)
    x = lax.rem(half + lax.div(group, 4) + lax.rem(group, 4) + 1, 2)
    return (2 * y + x, 2 * group + core)


def fine(src, stim, dst, low, count, kind, previous=None, before=None):
    u0 = src[0, low : low + count, :]
    u1 = src[1, low : low + count, :]
    v0 = src[2, low : low + count, :]
    v1 = src[3, low : low + count, :]

    def column(i):
        return src[i, low - 1 : low - 1 + count, :] + src[i, low + 1 : low + 1 + count, :]

    keep_u, keep_v, rate = KEEP_U, KEEP_V, 0.125
    if kind > 0:
        keep_u, keep_v, rate = KEEP_U - 4.0, KEEP_V - 4.0, 0.125 * 2**kind
    su0 = column(0) + (u1 + pltpu.roll(u1, 1, 1))
    su1 = column(1) + (u0 + pltpu.roll(u0, 127, 1))
    sv0 = column(2) + (v1 + pltpu.roll(v1, 1, 1))
    sv1 = column(3) + (v0 + pltpu.roll(v0, 127, 1))
    s0 = stim[4, low : low + count, :]
    s1 = stim[5, low : low + count, :]
    new = [
        (su0 + u0 * (keep_u - u0 * u0)) + (s0 - v0),
        (su1 + u1 * (keep_u - u1 * u1)) + (s1 - v1),
        sv0 + (keep_v * v0 + COUPLE * u0),
        sv1 + (keep_v * v1 + COUPLE * u1),
    ]
    for i in range(4):
        value = new[i] if rate == 1.0 else rate * new[i]
        if kind == 2:
            value = value - previous[i, low : low + count, :]
        if kind == 3:
            twice = previous[i, low : low + count, :]
            value = value - (twice + twice) - before[i, low : low + count, :]
        dst[i, low : low + count, :] = value


def kernel(
    u_in, v_in, s_in, u_out, v_out,
    loaded, rows, first, second, ping, pong, t_one, t_two, y_one, y_two, last, result,
    load_sem, in_send, in_recv, halo_send, halo_recv, out_send, out_recv,
):
    row, col = lax.axis_index("row"), lax.axis_index("col")
    y, x = lax.div(row, 2), lax.rem(row, 2)
    group, core = lax.div(col, 2), lax.rem(col, 2)
    turned = lax.rem(lax.div(group, 4) + lax.rem(group, 4) + 1, 2)
    half = lax.rem(x + turned, 2)
    spot = half * (4 + y) + (1 - half) * (3 - y)
    chip = 8 * group + spot
    own = half * 2 * y + (1 - half) * (6 - 2 * y) + core
    here = half == core
    across = lax.rem(core + turned, 2)

    inputs = (u_in, v_in, s_in)
    loads = [
        pltpu.make_async_copy(inputs[i], loaded.at[i], load_sem.at[i]) for i in range(3)
    ]
    for load in loads:
        load.start()

    left = place(lax.rem(chip + 63 + core, 64), 1 - core)
    right = place(lax.rem(chip + core, 64), 1 - core)

    def target(i):
        to_y = lax.rem(y + (2, 1, 3, 0)[i // 2], 4)
        to_core = lax.rem(core + 1 + i, 2)
        tile = core * 2 * to_y + (1 - core) * (6 - 2 * to_y) + to_core
        return (2 * to_y + across, 2 * group + to_core), tile

    def source(i):
        return lax.rem(row + i, 8)

    barrier = pltpu.get_barrier_semaphore()

    def greet(device):
        pl.semaphore_signal(barrier, inc=1, device_id=device, device_id_type=MESH)

    for i in range(7):
        greet(target(i)[0])
        greet((source(i + 1), 2 * group + half))

    @pl.when(jnp.logical_not(here))
    def _():
        greet(target(7)[0])
        greet((source(0), 2 * group + half))

    greet(left)
    greet(right)
    pl.semaphore_wait(barrier, 16 + 2 * (1 - jnp.where(here, 1, 0)))

    def lanes(tile):
        return pl.ds(pl.multiple_of(tile * 128, 128), 128)

    def piece(where):
        return pl.ds(pl.multiple_of(where * 32, 32), 32)

    def moved_in(field, i):
        device, tile = target(i)
        return pltpu.make_async_remote_copy(
            src_ref=loaded.at[field, :, lanes(tile)],
            dst_ref=rows.at[field, piece(row)],
            send_sem=in_send.at[field, i],
            recv_sem=in_recv.at[field, row],
            device_id=device,
            device_id_type=MESH,
        )

    def kept_in(field):
        return pltpu.make_async_copy(
            inputs[field].at[:, lanes(own)], rows.at[field, piece(row)], in_recv.at[field, row]
        )

    for field in range(3):
        loads[field].wait()
        for i in range(7):
            moved_in(field, i).start()

        @pl.when(here)
        def _():
            kept_in(field).start()

        @pl.when(jnp.logical_not(here))
        def _():
            moved_in(field, 7).start()

    def edge(buffer, planes, which, side):
        mine, theirs = ((HALO, WIDE - HALO), (WIDE - 2 * HALO, 0))[side]
        return pltpu.make_async_remote_copy(
            src_ref=buffer.at[planes, pl.ds(mine, HALO)],
            dst_ref=buffer.at[planes, pl.ds(theirs, HALO)],
            send_sem=halo_send.at[which, side],
            recv_sem=halo_recv.at[which, side],
            device_id=(left, right)[side],
            device_id_type=MESH,
        )

    edges = []
    for field in range(3):
        for sender in range(8):
            pltpu.make_async_copy(
                inputs[field].at[:, pl.ds(0, 128)],
                rows.at[field, pl.ds(32 * sender, 32)],
                in_recv.at[field, sender],
            ).wait()
        for parity in range(2):
            block = rows[field, pl.ds(parity, 128, stride=2), :].T
            if field == 0:
                block = block * (1.0 / SCALE)
            else:
                block = (block - SHIFT) * (0.4 / SCALE)
            first[2 * field + parity, HALO : HALO + STRIP, :] = block
        for side in range(2):
            copy = edge(first, pl.ds(2 * field, 2), field, side)
            copy.start()
            edges.append(copy)
    for copy in edges:
        copy.wait()

    start = first
    for outer in range(OUTER):
        done = 0
        state = start
        goal = (second, last)[outer]
        for top in range(TOP):
            for middle in range(MIDDLE):
                end = (t_one, t_two, (y_one, y_two, goal)[top])[middle]
                for micro in range(MICRO_COUNT):
                    done += 1
                    low = HALO - STEPS + done
                    count = -(-(WIDE - 2 * low) // 8) * 8
                    ends = micro == MICRO_COUNT - 1
                    kind = 0
                    if ends:
                        kind = 1 + (middle == MIDDLE - 1) * (1 + (top == TOP - 1))
                    into = end if ends else (ping, pong)[micro % 2]
                    fine(state, first, into, low, count, kind, t_two, y_two)
                    state = into
        start = goal
        if outer < OUTER - 1:
            edges = [edge(second, pl.ds(0, 4), 3 + outer, side) for side in range(2)]
            for copy in edges:
                copy.start()
            for copy in edges:
                copy.wait()

    outputs = (u_out, v_out)

    def moved_out(field, i):
        to = source(i)
        return pltpu.make_async_remote_copy(
            src_ref=result.at[field, piece(to)],
            dst_ref=outputs[field].at[:, lanes(own)],
            send_sem=out_send.at[field, i],
            recv_sem=out_recv.at[field, own],
            device_id=(to, 2 * group + half),
            device_id_type=MESH,
        )

    for field in range(2):
        for parity in range(2):
            block = last[2 * field + parity, HALO : HALO + STRIP, :]
            if field == 0:
                pass
            else:
                pass
            result[field, pl.ds(parity, 128, stride=2), :] = block.T
        for i in range(1, 8):
            moved_out(field, i).start()

        @pl.when(jnp.logical_not(here))
        def _():
            moved_out(field, 0).start()

        @pl.when(here)
        def _():
            outputs[field][:, lanes(own)] = result[field, piece(row), :]

    def arrived(field, tile):
        return pltpu.make_async_copy(
            result.at[field, pl.ds(0, 32)],
            outputs[field].at[:, pl.ds(0, 128)],
            out_recv.at[field, tile],
        )

    for field in range(2):
        for tile in range(8):

            @pl.when(jnp.logical_not(here) | (own != tile))
            def _():
                arrived(field, tile).wait()

    for field in range(3):
        for i in range(7):
            moved_in(field, i).wait_send()

        @pl.when(jnp.logical_not(here))
        def _():
            moved_in(field, 7).wait_send()

    for field in range(2):
        for i in range(1, 8):
            moved_out(field, i).wait_send()

        @pl.when(jnp.logical_not(here))
        def _():
            moved_out(field, 0).wait_send()


def body(u_field, v_field, stimulus):
    block = u_field.shape
    state = pltpu.VMEM((4, WIDE, 128), jnp.float32)
    u, v = pl.pallas_call(
        kernel,
        out_shape=[jax.ShapeDtypeStruct(block, jnp.float32)] * 2,
        in_specs=[pl.BlockSpec(memory_space=pltpu.HBM)] * 3,
        out_specs=[pl.BlockSpec(memory_space=pltpu.VMEM)] * 2,
        scratch_shapes=[
            pltpu.VMEM((3,) + block, jnp.float32),
            pltpu.VMEM((3, 256, STRIP), jnp.float32),
            pltpu.VMEM((6, WIDE, 128), jnp.float32),
            *[state] * 8,
            pltpu.VMEM((2, 256, STRIP), jnp.float32),
            pltpu.SemaphoreType.DMA((3,)),
            pltpu.SemaphoreType.DMA((3, 8)),
            pltpu.SemaphoreType.DMA((3, 8)),
            pltpu.SemaphoreType.DMA((4, 2)),
            pltpu.SemaphoreType.DMA((4, 2)),
            pltpu.SemaphoreType.DMA((2, 8)),
            pltpu.SemaphoreType.DMA((2, 8)),
        ],
        compiler_params=pltpu.CompilerParams(collective_id=0, has_side_effects=True, vmem_limit_bytes=12*1024*1024),
    )(*(pltpu.with_memory_space_constraint(a, pltpu.HBM) for a in (u_field, v_field, stimulus)))
    return u * SCALE, v * (SCALE / 0.4) + SHIFT


def solution(mesh):
    return jax.shard_map(
        body,
        mesh=mesh,
        in_specs=(P("row", "col"), P("row", "col"), P("row", "col")),
        out_specs=(P("row", "col"), P("row", "col")),
        check_vma=False,
    )
```

```python
import jax
import jax.numpy as jnp
from jax import lax
from jax.experimental import pallas as pl
from jax.experimental.pallas import tpu as pltpu
from jax.sharding import PartitionSpec as P

MESH = pl.DeviceIdType.MESH

MICRO_COUNT = 4
MIDDLE = 3
TOP = 3
OUTER = 2

SCALE = 7.5**0.5
SHIFT = 0.875
KEEP_U = 4.4
KEEP_V = 3.9744
COUPLE = 0.0128

STRIP = 128
HALO = 40
ORDER = (0, 1, 2, 3, 4, 5, 6, 7)
BLOCK = 16
STEPS = TOP * MIDDLE * MICRO_COUNT
WIDE = STRIP + 2 * HALO


def place(chip, core):
    group, spot = lax.div(chip, 8), lax.rem(chip, 8)
    upper = lax.div(group, 4)
    level = lax.div(spot, 2)
    back = lax.rem(group, 2)
    y = back * level + (1 - back) * (3 - level)
    x = lax.rem(1 - upper + lax.div(spot + 1, 2), 2)
    return (2 * y + x, 2 * group + core)


def plus(x):
    return pltpu.roll(x, 1, 1)


def minus(x):
    return pltpu.roll(x, 127, 1)


def lanes_summed(pairs, beside, plane, start, rows):
    for i in range(0, len(pairs), 2):
        even, odd = pairs[i], pairs[i + 1]
        beside[plane + i, start : start + rows, :] = odd + plus(odd)
        beside[plane + i + 1, start : start + rows, :] = even + minus(even)


def fine(src, beside, stim, dst, beside_next, low, count, micro, kind, previous, before):
    keep_u, keep_v = KEEP_U, KEEP_V
    if kind > 0:
        keep_u, keep_v = KEEP_U - 4.0, KEEP_V - 4.0
    cube = 1.0 / 64**micro
    rate = 0.125 * 2**kind / 8**micro
    for start in range(low, low + count, BLOCK):
        rows = min(BLOCK, low + count - start)

        def at(ref, plane, shift=0):
            return ref[plane, start + shift : start + shift + rows, :]

        u0, u1, v0, v1 = (at(src, i) for i in range(4))
        total = []
        for i in range(4):
            column = at(src, i, -1) + at(src, i, 1)
            total.append(column + at(beside, i))
        s0, s1 = at(stim, 2 * micro), at(stim, 2 * micro + 1)

        def bent(u):
            square = u * u
            return u * (keep_u - (square if micro == 0 else cube * square))

        new = [
            (total[0] + bent(u0)) + (s0 - v0),
            (total[1] + bent(u1)) + (s1 - v1),
            total[2] + (keep_v * v0 + COUPLE * u0),
            total[3] + (keep_v * v1 + COUPLE * u1),
        ]
        for i in range(4):
            if micro == MICRO_COUNT - 1:
                new[i] = rate * new[i]
            if kind == 2:
                new[i] = new[i] - at(previous, i)
            if kind == 3:
                twice = at(previous, i)
                new[i] = new[i] - (twice + twice) - at(before, i)
            dst[i, start : start + rows, :] = new[i]
        if beside_next is not None:
            lanes_summed(new, beside_next, 0, start, rows)


def kernel(
    u_in, v_in, s_in, u_out, v_out,
    loaded, rows, first, second, ping, pong, t_one, t_two, y_one, y_two, last,
    beside_one, beside_two, drive, result,
    load_sem, in_send, in_recv, halo_send, halo_recv, out_send, out_recv,
):
    row, col = lax.axis_index("row"), lax.axis_index("col")
    y, x = lax.div(row, 2), lax.rem(row, 2)
    group, core = lax.div(col, 2), lax.rem(col, 2)
    back = lax.rem(group, 2)
    level = back * y + (1 - back) * (3 - y)
    side = lax.rem(x + 1 - lax.div(group, 4), 2)
    spot = 2 * level + lax.rem(side + level, 2)
    half = lax.div(spot, 4)
    chip = 8 * group + spot
    own = 2 * (spot - 4 * half) + core
    here = half == core

    inputs = (u_in, v_in, s_in)
    loads = [
        pltpu.make_async_copy(inputs[i], loaded.at[i], load_sem.at[i]) for i in range(3)
    ]
    for load in loads:
        load.start()

    left = place(lax.rem(chip + 63 + core, 64), 1 - core)
    right = place(lax.rem(chip + core, 64), 1 - core)

    def target(i):
        tile = lax.rem(own + 1 + i, 8)
        return place(8 * group + 4 * core + lax.div(tile, 2), lax.rem(tile, 2)), tile

    def source(i):
        return lax.rem(row + i, 8)

    barrier = pltpu.get_barrier_semaphore()

    def greet(device):
        pl.semaphore_signal(barrier, inc=1, device_id=device, device_id_type=MESH)

    for i in range(7):
        greet(target(i)[0])
        greet((source(i + 1), 2 * group + half))

    @pl.when(jnp.logical_not(here))
    def _():
        greet(target(7)[0])
        greet((source(0), 2 * group + half))

    greet(left)
    greet(right)
    pl.semaphore_wait(barrier, 16 + 2 * (1 - jnp.where(here, 1, 0)))

    def lanes(tile):
        return pl.ds(pl.multiple_of(tile * 128, 128), 128)

    def piece(where):
        return pl.ds(pl.multiple_of(where * 32, 32), 32)

    def moved_in(field, i):
        device, tile = target(i)
        return pltpu.make_async_remote_copy(
            src_ref=loaded.at[field, :, lanes(tile)],
            dst_ref=rows.at[field, piece(row)],
            send_sem=in_send,
            recv_sem=in_recv.at[field],
            device_id=device,
            device_id_type=MESH,
        )

    def kept_in(field):
        return pltpu.make_async_copy(
            inputs[field].at[:, lanes(own)], rows.at[field, piece(row)], in_recv.at[field]
        )

    for field in range(3):
        loads[field].wait()
        for i in range(7):
            moved_in(field, i).start()

        @pl.when(here)
        def _():
            kept_in(field).start()

        @pl.when(jnp.logical_not(here))
        def _():
            moved_in(field, 7).start()

    def edge(buffer, planes, which, side):
        mine, theirs = ((HALO, WIDE - HALO), (WIDE - 2 * HALO, 0))[side]
        return pltpu.make_async_remote_copy(
            src_ref=buffer.at[planes, pl.ds(mine, HALO)],
            dst_ref=buffer.at[planes, pl.ds(theirs, HALO)],
            send_sem=halo_send.at[which, side],
            recv_sem=halo_recv.at[which, side],
            device_id=(left, right)[side],
            device_id_type=MESH,
        )

    edges = []
    for field in range(3):
        pltpu.make_async_copy(rows.at[field], rows.at[field], in_recv.at[field]).wait()
        for parity in range(2):
            block = rows[field, pl.ds(parity, 128, stride=2), :].T
            if field == 0:
                block = block * (1.0 / SCALE)
            else:
                block = (block - SHIFT) * (0.4 / SCALE)
            first[2 * field + parity, HALO : HALO + STRIP, :] = block
        for side in range(2):
            copy = edge(first, pl.ds(2 * field, 2), field, side)
            copy.start()
            edges.append(copy)
        if field < 2:
            pair = [first[2 * field + parity, HALO : HALO + STRIP, :] for parity in range(2)]
            lanes_summed(pair, beside_one, 2 * field, HALO, STRIP)

    def halos_summed(state):
        @pl.when(row >= 0)
        def _():
            for low in (0, HALO + STRIP):
                planes = [state[i, low : low + HALO, :] for i in range(4)]
                lanes_summed(planes, beside_one, 0, low, HALO)

    for copy in edges:
        copy.wait()
    for micro in range(MICRO_COUNT):
        for parity in range(2):
            drive[2 * micro + parity, :, :] = 8.0**micro * first[4 + parity, :, :]

    halos_summed(first)
    start = first
    for outer in range(OUTER):
        done = 0
        state = start
        goal = (second, last)[outer]
        for top in range(TOP):
            for middle in range(MIDDLE):
                end = (t_one, t_two, (y_one, y_two, goal)[top])[middle]
                for micro in range(MICRO_COUNT):
                    done += 1
                    low = HALO - STEPS + done
                    count = -(-(WIDE - 2 * low) // 8) * 8
                    ends = micro == MICRO_COUNT - 1
                    kind = 0
                    if ends:
                        kind = 1 + (middle == MIDDLE - 1) * (1 + (top == TOP - 1))
                    into = end if ends else (ping, pong)[micro % 2]
                    beside = (beside_two, beside_one)[done % 2]
                    beside_next = (beside_one, beside_two)[done % 2]
                    if done == STEPS and outer == OUTER - 1:
                        beside_next = None
                    fine(
                        state, beside, drive, into, beside_next,
                        low, count, micro, kind, t_two, y_two,
                    )
                    state = into
        start = goal
        if outer < OUTER - 1:
            edges = [edge(second, pl.ds(0, 4), 3 + outer, side) for side in range(2)]
            for copy in edges:
                copy.start()
            for copy in edges:
                copy.wait()
            halos_summed(second)

    outputs = (u_out, v_out)

    def moved_out(field, to):
        return pltpu.make_async_remote_copy(
            src_ref=result.at[field, pl.ds(32 * to, 32)],
            dst_ref=outputs[field].at[:, lanes(own)],
            send_sem=out_send,
            recv_sem=out_recv,
            device_id=(jnp.int32(to), 2 * group + half),
            device_id_type=MESH,
        )

    for field in range(2):
        for parity in range(2):
            block = last[2 * field + parity, HALO : HALO + STRIP, :]
            result[field, pl.ds(parity, 128, stride=2), :] = block.T
    for to in ORDER:

        @pl.when(jnp.logical_not(here) | (row != to))
        def _():
            moved_out(0, to).start()
            moved_out(1, to).start()

    @pl.when(here)
    def _():
        for field in range(2):
            outputs[field][:, lanes(own)] = result[field, piece(row), :]

    def settle(count):
        for buffer, semaphore in ((result, out_recv), (rows, in_send), (result, out_send)):
            part = buffer.at[:, pl.ds(0, 32 * count)]
            pltpu.make_async_copy(part, part, semaphore).wait()

    @pl.when(here)
    def _():
        settle(7)

    @pl.when(jnp.logical_not(here))
    def _():
        settle(8)


def body(u_field, v_field, stimulus):
    block = u_field.shape
    state = pltpu.VMEM((4, WIDE, 128), jnp.float32)
    u, v = pl.pallas_call(
        kernel,
        out_shape=[jax.ShapeDtypeStruct(block, jnp.float32)] * 2,
        in_specs=[pl.BlockSpec(memory_space=pltpu.HBM)] * 3,
        out_specs=[pl.BlockSpec(memory_space=pltpu.VMEM)] * 2,
        scratch_shapes=[
            pltpu.VMEM((3,) + block, jnp.float32),
            pltpu.VMEM((3, 256, STRIP), jnp.float32),
            pltpu.VMEM((6, WIDE, 128), jnp.float32),
            *[state] * 10,
            pltpu.VMEM((2 * MICRO_COUNT, WIDE, 128), jnp.float32),
            pltpu.VMEM((2, 256, STRIP), jnp.float32),
            pltpu.SemaphoreType.DMA((3,)),
            pltpu.SemaphoreType.DMA,
            pltpu.SemaphoreType.DMA((3,)),
            pltpu.SemaphoreType.DMA((4, 2)),
            pltpu.SemaphoreType.DMA((4, 2)),
            pltpu.SemaphoreType.DMA,
            pltpu.SemaphoreType.DMA,
        ],
        compiler_params=pltpu.CompilerParams(collective_id=0, has_side_effects=True, vmem_limit_bytes=12*1024*1024),
    )(*(pltpu.with_memory_space_constraint(a, pltpu.HBM) for a in (u_field, v_field, stimulus)))
    return u * SCALE, v * (SCALE / 0.4) + SHIFT


def solution(mesh):
    return jax.shard_map(
        body,
        mesh=mesh,
        in_specs=(P("row", "col"), P("row", "col"), P("row", "col")),
        out_specs=(P("row", "col"), P("row", "col")),
        check_vma=False,
    )
```

```python
import jax
import jax.numpy as jnp
from jax import lax
from jax.experimental import pallas as pl
from jax.experimental.pallas import tpu as pltpu
from jax.sharding import PartitionSpec as P

MESH = pl.DeviceIdType.MESH

MICRO_COUNT = 4
MIDDLE = 3
TOP = 3
OUTER = 2

SCALE = 7.5**0.5
SHIFT = 0.875
KEEP_U = 4.4
KEEP_V = 3.9744
COUPLE = 0.0128

STRIP = 128
HALO = 40
ORDER = (0, 1, 2, 3, 4, 5, 6, 7)
BLOCK = 16
STEPS = TOP * MIDDLE * MICRO_COUNT
WIDE = STRIP + 2 * HALO


def swapped(group):
    return 1 - lax.div(lax.rem(group, 4), 2)


def place(chip, side):
    group, spot = lax.div(chip, 8), lax.rem(chip, 8)
    upper = lax.div(group, 4)
    level = lax.div(spot, 2)
    back = lax.rem(group, 2)
    y = back * level + (1 - back) * (3 - level)
    x = lax.rem(1 - upper + lax.div(spot + 1, 2), 2)
    return (2 * y + x, 2 * group + lax.rem(side + swapped(group), 2))


def plus(x):
    return pltpu.roll(x, 1, 1)


def minus(x):
    return pltpu.roll(x, 127, 1)


def lanes_summed(pairs, beside, plane, start, rows):
    for i in range(0, len(pairs), 2):
        even, odd = pairs[i], pairs[i + 1]
        beside[plane + i, start : start + rows, :] = odd + plus(odd)
        beside[plane + i + 1, start : start + rows, :] = even + minus(even)


def fine(src, beside, stim, dst, beside_next, low, count, micro, kind, previous, before):
    keep_u, keep_v = KEEP_U, KEEP_V
    if kind > 0:
        keep_u, keep_v = KEEP_U - 4.0, KEEP_V - 4.0
    cube = 1.0 / 64**micro
    rate = 0.125 * 2**kind / 8**micro
    for start in range(low, low + count, BLOCK):
        rows = min(BLOCK, low + count - start)

        def at(ref, plane, shift=0):
            return ref[plane, start + shift : start + shift + rows, :]

        u0, u1, v0, v1 = (at(src, i) for i in range(4))
        total = []
        for i in range(4):
            column = at(src, i, -1) + at(src, i, 1)
            total.append(column + at(beside, i))
        s0, s1 = at(stim, 2 * micro), at(stim, 2 * micro + 1)

        def bent(u):
            square = u * u
            return u * (keep_u - (square if micro == 0 else cube * square))

        new = [
            (total[0] + bent(u0)) + (s0 - v0),
            (total[1] + bent(u1)) + (s1 - v1),
            total[2] + (keep_v * v0 + COUPLE * u0),
            total[3] + (keep_v * v1 + COUPLE * u1),
        ]
        for i in range(4):
            if micro == MICRO_COUNT - 1:
                new[i] = rate * new[i]
            if kind == 2:
                new[i] = new[i] - at(previous, i)
            if kind == 3:
                twice = at(previous, i)
                new[i] = new[i] - (twice + twice) - at(before, i)
            dst[i, start : start + rows, :] = new[i]
        if beside_next is not None:
            lanes_summed(new, beside_next, 0, start, rows)


def kernel(
    u_in, v_in, s_in, u_out, v_out,
    loaded, rows, first, second, ping, pong, t_one, t_two, y_one, y_two, last,
    beside_one, beside_two, drive, result,
    load_sem, in_send, in_recv, halo_send, halo_recv, out_send, out_recv,
):
    row, col = lax.axis_index("row"), lax.axis_index("col")
    y, x = lax.div(row, 2), lax.rem(row, 2)
    group, core = lax.div(col, 2), lax.rem(col, 2)
    back = lax.rem(group, 2)
    level = back * y + (1 - back) * (3 - y)
    side = lax.rem(x + 1 - lax.div(group, 4), 2)
    spot = 2 * level + lax.rem(side + level, 2)
    half = lax.div(spot, 4)
    chip = 8 * group + spot
    hand = lax.rem(core + swapped(group), 2)
    own = 2 * (spot - 4 * half) + hand
    here = half == core

    inputs = (u_in, v_in, s_in)
    loads = [
        pltpu.make_async_copy(inputs[i], loaded.at[i], load_sem.at[i]) for i in range(3)
    ]
    for load in loads:
        load.start()

    left = place(lax.rem(chip + 63 + hand, 64), 1 - hand)
    right = place(lax.rem(chip + hand, 64), 1 - hand)

    def target(i):
        tile = lax.rem(own + 1 + i, 8)
        return place(8 * group + 4 * core + lax.div(tile, 2), lax.rem(tile, 2)), tile

    def source(i):
        return lax.rem(row + i, 8)

    barrier = pltpu.get_barrier_semaphore()

    def greet(device):
        pl.semaphore_signal(barrier, inc=1, device_id=device, device_id_type=MESH)

    for i in range(1, 8):
        greet((source(i), 2 * group + half))

    @pl.when(jnp.logical_not(here))
    def _():
        greet((row, 2 * group + half))

    for i in range(4):
        to_row = place(8 * group + 4 * core + i, 0)[0]
        greet((to_row, 2 * group + 1 - half))
    greet(left)
    greet(right)
    pl.semaphore_wait(barrier, 14 - jnp.where(here, 1, 0))

    def lanes(tile):
        return pl.ds(pl.multiple_of(tile * 128, 128), 128)

    def piece(where):
        return pl.ds(pl.multiple_of(where * 32, 32), 32)

    def moved_in(field, i):
        device, tile = target(i)
        return pltpu.make_async_remote_copy(
            src_ref=loaded.at[field, :, lanes(tile)],
            dst_ref=rows.at[field, piece(row)],
            send_sem=in_send,
            recv_sem=in_recv.at[field],
            device_id=device,
            device_id_type=MESH,
        )

    def kept_in(field):
        return pltpu.make_async_copy(
            inputs[field].at[:, lanes(own)], rows.at[field, piece(row)], in_recv.at[field]
        )

    for field in range(3):
        loads[field].wait()
        for i in range(7):
            moved_in(field, i).start()

        @pl.when(here)
        def _():
            kept_in(field).start()

        @pl.when(jnp.logical_not(here))
        def _():
            moved_in(field, 7).start()

    def edge(buffer, planes, which, side):
        mine, theirs = ((HALO, WIDE - HALO), (WIDE - 2 * HALO, 0))[side]
        return pltpu.make_async_remote_copy(
            src_ref=buffer.at[planes, pl.ds(mine, HALO)],
            dst_ref=buffer.at[planes, pl.ds(theirs, HALO)],
            send_sem=halo_send.at[which, side],
            recv_sem=halo_recv.at[which, side],
            device_id=(left, right)[side],
            device_id_type=MESH,
        )

    edges = []
    for field in range(3):
        pltpu.make_async_copy(rows.at[field], rows.at[field], in_recv.at[field]).wait()
        for parity in range(2):
            block = rows[field, pl.ds(parity, 128, stride=2), :].T
            if field == 0:
                block = block * (1.0 / SCALE)
            else:
                block = (block - SHIFT) * (0.4 / SCALE)
            first[2 * field + parity, HALO : HALO + STRIP, :] = block
        for side in range(2):
            copy = edge(first, pl.ds(2 * field, 2), field, side)
            copy.start()
            edges.append(copy)
        if field < 2:
            pair = [first[2 * field + parity, HALO : HALO + STRIP, :] for parity in range(2)]
            lanes_summed(pair, beside_one, 2 * field, HALO, STRIP)

    def halos_summed(state):
        @pl.when(row >= 0)
        def _():
            for low in (0, HALO + STRIP):
                planes = [state[i, low : low + HALO, :] for i in range(4)]
                lanes_summed(planes, beside_one, 0, low, HALO)

    for copy in edges:
        copy.wait()
    for micro in range(MICRO_COUNT):
        for parity in range(2):
            drive[2 * micro + parity, :, :] = 8.0**micro * first[4 + parity, :, :]

    halos_summed(first)
    start = first
    for outer in range(OUTER):
        done = 0
        state = start
        goal = (second, last)[outer]
        for top in range(TOP):
            for middle in range(MIDDLE):
                end = (t_one, t_two, (y_one, y_two, goal)[top])[middle]
                for micro in range(MICRO_COUNT):
                    done += 1
                    low = HALO - STEPS + done
                    count = -(-(WIDE - 2 * low) // 8) * 8
                    ends = micro == MICRO_COUNT - 1
                    kind = 0
                    if ends:
                        kind = 1 + (middle == MIDDLE - 1) * (1 + (top == TOP - 1))
                    into = end if ends else (ping, pong)[micro % 2]
                    beside = (beside_two, beside_one)[done % 2]
                    beside_next = (beside_one, beside_two)[done % 2]
                    if done == STEPS and outer == OUTER - 1:
                        beside_next = None
                    fine(
                        state, beside, drive, into, beside_next,
                        low, count, micro, kind, t_two, y_two,
                    )
                    state = into
        start = goal
        if outer < OUTER - 1:
            edges = [edge(second, pl.ds(0, 4), 3 + outer, side) for side in range(2)]
            for copy in edges:
                copy.start()
            for copy in edges:
                copy.wait()
            halos_summed(second)

    outputs = (u_out, v_out)

    def moved_out(field, to):
        return pltpu.make_async_remote_copy(
            src_ref=result.at[field, pl.ds(32 * to, 32)],
            dst_ref=outputs[field].at[:, lanes(own)],
            send_sem=out_send,
            recv_sem=out_recv,
            device_id=(jnp.int32(to), 2 * group + half),
            device_id_type=MESH,
        )

    for field in range(2):
        for parity in range(2):
            block = last[2 * field + parity, HALO : HALO + STRIP, :]
            result[field, pl.ds(parity, 128, stride=2), :] = block.T
    for to in ORDER:

        @pl.when(jnp.logical_not(here) | (row != to))
        def _():
            moved_out(0, to).start()
            moved_out(1, to).start()

    @pl.when(here)
    def _():
        for field in range(2):
            outputs[field][:, lanes(own)] = result[field, piece(row), :]

    def settle(count):
        for buffer, semaphore in ((result, out_recv), (rows, in_send), (result, out_send)):
            part = buffer.at[:, pl.ds(0, 32 * count)]
            pltpu.make_async_copy(part, part, semaphore).wait()

    @pl.when(here)
    def _():
        settle(7)

    @pl.when(jnp.logical_not(here))
    def _():
        settle(8)


def body(u_field, v_field, stimulus):
    block = u_field.shape
    state = pltpu.VMEM((4, WIDE, 128), jnp.float32)
    u, v = pl.pallas_call(
        kernel,
        out_shape=[jax.ShapeDtypeStruct(block, jnp.float32)] * 2,
        in_specs=[pl.BlockSpec(memory_space=pltpu.HBM)] * 3,
        out_specs=[pl.BlockSpec(memory_space=pltpu.VMEM)] * 2,
        scratch_shapes=[
            pltpu.VMEM((3,) + block, jnp.float32),
            pltpu.VMEM((3, 256, STRIP), jnp.float32),
            pltpu.VMEM((6, WIDE, 128), jnp.float32),
            *[state] * 10,
            pltpu.VMEM((2 * MICRO_COUNT, WIDE, 128), jnp.float32),
            pltpu.VMEM((2, 256, STRIP), jnp.float32),
            pltpu.SemaphoreType.DMA((3,)),
            pltpu.SemaphoreType.DMA,
            pltpu.SemaphoreType.DMA((3,)),
            pltpu.SemaphoreType.DMA((4, 2)),
            pltpu.SemaphoreType.DMA((4, 2)),
            pltpu.SemaphoreType.DMA,
            pltpu.SemaphoreType.DMA,
        ],
        compiler_params=pltpu.CompilerParams(collective_id=0, has_side_effects=True, vmem_limit_bytes=12*1024*1024),
    )(*(pltpu.with_memory_space_constraint(a, pltpu.HBM) for a in (u_field, v_field, stimulus)))
    return u * SCALE, v * (SCALE / 0.4) + SHIFT


def solution(mesh):
    return jax.shard_map(
        body,
        mesh=mesh,
        in_specs=(P("row", "col"), P("row", "col"), P("row", "col")),
        out_specs=(P("row", "col"), P("row", "col")),
        check_vma=False,
    )
```

```python
import jax
import jax.numpy as jnp
from jax import lax
from jax.experimental import pallas as pl
from jax.experimental.pallas import tpu as pltpu
from jax.sharding import PartitionSpec as P

MESH = pl.DeviceIdType.MESH

MICRO_COUNT = 4
MIDDLE = 3
TOP = 3
OUTER = 2

SCALE = 7.5**0.5
SHIFT = 0.875
KEEP_U = 4.4
KEEP_V = 3.9744
COUPLE = 0.0128

STRIP = 128
HALO = 40
ORDER = (0, 1, 2, 3, 4, 5, 6, 7)
BLOCK = 16
STEPS = TOP * MIDDLE * MICRO_COUNT
WIDE = STRIP + 2 * HALO
PLANE = WIDE + 8


def swapped(group):
    return 1 - lax.div(lax.rem(group, 4), 2)


def place(chip, side):
    group, spot = lax.div(chip, 8), lax.rem(chip, 8)
    upper = lax.div(group, 4)
    level = lax.div(spot, 2)
    back = lax.rem(group, 2)
    y = back * level + (1 - back) * (3 - level)
    x = lax.rem(1 - upper + lax.div(spot + 1, 2), 2)
    return (2 * y + x, 2 * group + lax.rem(side + swapped(group), 2))


def plus(x):
    return pltpu.roll(x, 1, 1)


def minus(x):
    return pltpu.roll(x, 127, 1)


def lanes_summed(pairs, beside, plane, start, rows):
    for i in range(0, len(pairs), 2):
        even, odd = pairs[i], pairs[i + 1]
        beside[plane + i, start : start + rows, :] = odd + plus(odd)
        beside[plane + i + 1, start : start + rows, :] = even + minus(even)


def fine(src, beside, stim, dst, beside_next, low, count, micro, kind, previous, before):
    keep_u, keep_v = KEEP_U, KEEP_V
    if kind > 0:
        keep_u, keep_v = KEEP_U - 4.0, KEEP_V - 4.0
    cube = 1.0 / 64**micro
    rate = 0.125 * 2**kind / 8**micro
    for start in range(low, low + count, BLOCK):
        rows = min(BLOCK, low + count - start)

        def at(ref, plane, shift=0):
            return ref[plane, start + shift : start + shift + rows, :]

        u0, u1, v0, v1 = (at(src, i) for i in range(4))
        total = []
        for i in range(4):
            column = at(src, i, -1) + at(src, i, 1)
            total.append(column + at(beside, i))
        s0, s1 = at(stim, 2 * micro), at(stim, 2 * micro + 1)

        def bent(u):
            square = u * u
            return u * (keep_u - (square if micro == 0 else cube * square))

        new = [
            (total[0] + bent(u0)) + (s0 - v0),
            (total[1] + bent(u1)) + (s1 - v1),
            total[2] + (keep_v * v0 + COUPLE * u0),
            total[3] + (keep_v * v1 + COUPLE * u1),
        ]
        for i in range(4):
            if micro == MICRO_COUNT - 1:
                new[i] = rate * new[i]
            if kind == 2:
                new[i] = new[i] - at(previous, i)
            if kind == 3:
                twice = at(previous, i)
                new[i] = new[i] - (twice + twice) - at(before, i)
            dst[i, start : start + rows, :] = new[i]
        if beside_next is not None:
            lanes_summed(new, beside_next, 0, start, rows)


def kernel(
    u_in, v_in, s_in, u_out, v_out,
    loaded, rows, first, second, ping, pong, t_one, t_two, y_one, y_two, last,
    beside_one, beside_two, drive, result,
    load_sem, in_send, in_recv, halo_send, halo_recv, out_send, out_recv,
):
    row, col = lax.axis_index("row"), lax.axis_index("col")
    y, x = lax.div(row, 2), lax.rem(row, 2)
    group, core = lax.div(col, 2), lax.rem(col, 2)
    back = lax.rem(group, 2)
    level = back * y + (1 - back) * (3 - y)
    side = lax.rem(x + 1 - lax.div(group, 4), 2)
    spot = 2 * level + lax.rem(side + level, 2)
    half = lax.div(spot, 4)
    chip = 8 * group + spot
    hand = lax.rem(core + swapped(group), 2)
    own = 2 * (spot - 4 * half) + hand
    here = half == core

    inputs = (u_in, v_in, s_in)
    loads = [
        pltpu.make_async_copy(inputs[i], loaded.at[i], load_sem.at[i]) for i in range(3)
    ]
    for load in loads:
        load.start()

    left = place(lax.rem(chip + 63 + hand, 64), 1 - hand)
    right = place(lax.rem(chip + hand, 64), 1 - hand)

    def target(i):
        tile = lax.rem(own + 1 + i, 8)
        return place(8 * group + 4 * core + lax.div(tile, 2), lax.rem(tile, 2)), tile

    def source(i):
        return lax.rem(row + i, 8)

    barrier = pltpu.get_barrier_semaphore()

    def greet(device):
        pl.semaphore_signal(barrier, inc=1, device_id=device, device_id_type=MESH)

    for i in range(1, 8):
        greet((source(i), 2 * group + half))

    @pl.when(jnp.logical_not(here))
    def _():
        greet((row, 2 * group + half))

    for i in range(4):
        to_row = place(8 * group + 4 * core + i, 0)[0]
        greet((to_row, 2 * group + 1 - half))
    greet(left)
    greet(right)
    pl.semaphore_wait(barrier, 14 - jnp.where(here, 1, 0))

    def lanes(tile):
        return pl.ds(pl.multiple_of(tile * 128, 128), 128)

    def piece(where):
        return pl.ds(pl.multiple_of(where * 32, 32), 32)

    def moved_in(field, i):
        device, tile = target(i)
        return pltpu.make_async_remote_copy(
            src_ref=loaded.at[field, :, lanes(tile)],
            dst_ref=rows.at[field, piece(row)],
            send_sem=in_send,
            recv_sem=in_recv.at[field],
            device_id=device,
            device_id_type=MESH,
        )

    def kept_in(field):
        return pltpu.make_async_copy(
            inputs[field].at[:, lanes(own)], rows.at[field, piece(row)], in_recv.at[field]
        )

    for field in range(3):
        loads[field].wait()
        for i in range(7):
            moved_in(field, i).start()

        @pl.when(here)
        def _():
            kept_in(field).start()

        @pl.when(jnp.logical_not(here))
        def _():
            moved_in(field, 7).start()

    def edge(buffer, planes, which, side):
        mine, theirs = ((HALO, WIDE - HALO), (WIDE - 2 * HALO, 0))[side]
        return pltpu.make_async_remote_copy(
            src_ref=buffer.at[planes, pl.ds(mine, HALO)],
            dst_ref=buffer.at[planes, pl.ds(theirs, HALO)],
            send_sem=halo_send.at[which],
            recv_sem=halo_recv.at[which],
            device_id=(left, right)[side],
            device_id_type=MESH,
        )

    def driven(low, count):
        for micro in range(MICRO_COUNT):
            for parity in range(2):
                value = first[4 + parity, low : low + count, :]
                drive[2 * micro + parity, low : low + count, :] = 8.0**micro * value

    def edges_of(buffer):
        return buffer.at[:, pl.ds(0, 2 * HALO)]

    for field in range(3):
        pltpu.make_async_copy(rows.at[field], rows.at[field], in_recv.at[field]).wait()
        for parity in range(2):
            block = rows[field, pl.ds(parity, 128, stride=2), :].T
            if field == 0:
                block = block * (1.0 / SCALE)
            else:
                block = (block - SHIFT) * (0.4 / SCALE)
            first[2 * field + parity, HALO : HALO + STRIP, :] = block
        for side in range(2):
            edge(first, pl.ds(2 * field, 2), 0, side).start()
        if field < 2:
            pair = [first[2 * field + parity, HALO : HALO + STRIP, :] for parity in range(2)]
            lanes_summed(pair, beside_one, 2 * field, HALO, STRIP)
        else:
            driven(HALO, STRIP)

    def halos_summed(state):
        @pl.when(row >= 0)
        def _():
            for low in (0, HALO + STRIP):
                planes = [state[i, low : low + HALO, :] for i in range(4)]
                lanes_summed(planes, beside_one, 0, low, HALO)

    pltpu.make_async_copy(edges_of(first), edges_of(first), halo_recv.at[0]).wait()
    driven(0, HALO)
    driven(HALO + STRIP, HALO)
    halos_summed(first)
    start = first
    for outer in range(OUTER):
        done = 0
        state = start
        goal = (second, last)[outer]
        for top in range(TOP):
            for middle in range(MIDDLE):
                end = (t_one, t_two, (y_one, y_two, goal)[top])[middle]
                for micro in range(MICRO_COUNT):
                    done += 1
                    low = HALO - STEPS + done
                    count = -(-(WIDE - 2 * low) // 8) * 8
                    ends = micro == MICRO_COUNT - 1
                    kind = 0
                    if ends:
                        kind = 1 + (middle == MIDDLE - 1) * (1 + (top == TOP - 1))
                    into = end if ends else (ping, pong)[micro % 2]
                    beside = (beside_two, beside_one)[done % 2]
                    beside_next = (beside_one, beside_two)[done % 2]
                    if done == STEPS and outer == OUTER - 1:
                        beside_next = None
                    fine(
                        state, beside, drive, into, beside_next,
                        low, count, micro, kind, t_two, y_two,
                    )
                    state = into
        start = goal
        if outer < OUTER - 1:
            for side in range(2):
                edge(second, pl.ds(0, 4), 1, side).start()
            pltpu.make_async_copy(edges_of(second), edges_of(second), halo_recv.at[1]).wait()
            halos_summed(second)

    outputs = (u_out, v_out)

    def moved_out(field, to):
        return pltpu.make_async_remote_copy(
            src_ref=result.at[field, pl.ds(32 * to, 32)],
            dst_ref=outputs[field].at[:, lanes(own)],
            send_sem=out_send,
            recv_sem=out_recv,
            device_id=(jnp.int32(to), 2 * group + half),
            device_id_type=MESH,
        )

    for field in range(2):
        for parity in range(2):
            block = last[2 * field + parity, HALO : HALO + STRIP, :]
            result[field, pl.ds(parity, 128, stride=2), :] = block.T
    for to in ORDER:

        @pl.when(jnp.logical_not(here) | (row != to))
        def _():
            moved_out(0, to).start()
            moved_out(1, to).start()

    @pl.when(here)
    def _():
        for field in range(2):
            outputs[field][:, lanes(own)] = result[field, piece(row), :]

    def settle(count):
        for buffer, semaphore in ((result, out_recv), (rows, in_send), (result, out_send)):
            part = buffer.at[:, pl.ds(0, 32 * count)]
            pltpu.make_async_copy(part, part, semaphore).wait()

    pltpu.make_async_copy(edges_of(first), edges_of(first), halo_send.at[0]).wait()
    pltpu.make_async_copy(edges_of(second), edges_of(second), halo_send.at[1]).wait()

    @pl.when(here)
    def _():
        settle(7)

    @pl.when(jnp.logical_not(here))
    def _():
        settle(8)


def body(u_field, v_field, stimulus):
    block = u_field.shape
    state = pltpu.VMEM((4, PLANE, 128), jnp.float32)
    u, v = pl.pallas_call(
        kernel,
        out_shape=[jax.ShapeDtypeStruct(block, jnp.float32)] * 2,
        in_specs=[pl.BlockSpec(memory_space=pltpu.HBM)] * 3,
        out_specs=[pl.BlockSpec(memory_space=pltpu.VMEM)] * 2,
        scratch_shapes=[
            pltpu.VMEM((3,) + block, jnp.float32),
            pltpu.VMEM((3, 256, STRIP), jnp.float32),
            pltpu.VMEM((6, PLANE, 128), jnp.float32),
            *[state] * 10,
            pltpu.VMEM((2 * MICRO_COUNT, PLANE, 128), jnp.float32),
            pltpu.VMEM((2, 256, STRIP), jnp.float32),
            pltpu.SemaphoreType.DMA((3,)),
            pltpu.SemaphoreType.DMA,
            pltpu.SemaphoreType.DMA((3,)),
            pltpu.SemaphoreType.DMA((2,)),
            pltpu.SemaphoreType.DMA((2,)),
            pltpu.SemaphoreType.DMA,
            pltpu.SemaphoreType.DMA,
        ],
        compiler_params=pltpu.CompilerParams(collective_id=0, has_side_effects=True, vmem_limit_bytes=12*1024*1024),
    )(*(pltpu.with_memory_space_constraint(a, pltpu.HBM) for a in (u_field, v_field, stimulus)))
    return u * SCALE, v * (SCALE / 0.4) + SHIFT


def solution(mesh):
    return jax.shard_map(
        body,
        mesh=mesh,
        in_specs=(P("row", "col"), P("row", "col"), P("row", "col")),
        out_specs=(P("row", "col"), P("row", "col")),
        check_vma=False,
    )
```
